256 devices in a mesh: dp: 128 (over y, x_hi, z, core), tensor: 2 (over x_lo).
Axes of the slice: x: 4 (x_hi: 2, x_lo: 2; x = x_hi * 2 + x_lo), y: 4, z: 8, core: 2. Of those that a mesh axis runs over, the one named last changes fastest.
Arguments:
- query_feats: bfloat16 [32768, 768], P('dp'), may hold values from -24 to 24
- key_feats: bfloat16 [512, 768], P('dp'), may hold values from -6 to 6
- key_task: int32 [512], P('dp'), may hold values from 0 to 3
- positive: int32 [32768], P('dp'), may hold values from 0 to 511
- head_weights: bfloat16 [4, 768, 768], P(None, None, 'tensor'), may hold values from -0.21875 to 0.21875
- task_scale: float32 [4], replicated, may hold values from 10 to 30
Outputs:
- query_loss: float32 [32768], P(('dp', 'tensor'))
- weight_grad: float32 [4, 768, 768], P(None, 'dp', 'tensor')
The draws below stay inside these ranges and needn't reach their ends.
All inputs are finite; a program needn't handle non-finite values.
Results may differ from the reference program's by a relative error of at most 0.0075.
Values may be sent and summed in bfloat16 or wider, within the bound.
No kernel may reach another device: no remote copies, remote signals or barrier semaphores. Data moves between devices by JAX's collectives and lax.ppermute only.
A program may use at most 64 MiB of HBM per device.

```python
import math
import jax
import jax.numpy as jnp
from jax import lax

D = 768
E = 768
TASKS = 4
QUERIES = 32768
KEYS = 512


def with_ends(drawn, rng, least, top_value):
    dims = drawn.shape
    spot = [jax.random.randint(jax.random.fold_in(rng, axis), (), 0, dims[axis]) for axis in range(len(dims))]
    drawn = drawn.at[tuple(spot)].set(least)
    longest = dims.index(max(dims))
    spot[longest] = (spot[longest] + 1) % dims[longest]
    return drawn.at[tuple(spot)].set(top_value)


def with_spikes(array, own_key, source, target, shards_of, factor):
    def block_of(dim):
        return (jnp.arange(array.shape[dim]) // (array.shape[dim] // shards_of)).reshape((-1,) + (1,) * (array.ndim - 1 - dim))

    first = jax.random.permutation(own_key, shards_of)[block_of(target)]
    second = (block_of(target) + shards_of // 2) % shards_of
    return jnp.where((block_of(source) == first) | (block_of(source) == second), factor * array, array)


def shard_levels(key, dims, split, least, largest):
    def one(axis_at, blocks):
        heights = jax.random.uniform(jax.random.fold_in(jax.random.fold_in(key, 6), axis_at), (blocks,), jnp.float32, least / len(split), largest / len(split))
        return jnp.repeat(jnp.exp(heights), dims[axis_at] // blocks).reshape((-1,) + (1,) * (len(dims) - axis_at - 1))

    factor_of = one(*split[0])
    for cut in split[1:]:
        factor_of = factor_of * one(*cut)
    return factor_of


def gaussian(own_key, shape, width, reach, split=(), dtype=jnp.bfloat16):
    level = shard_levels(own_key, shape, split, -0.22, 0.18) if split else 1.0
    values = jax.random.normal(own_key, shape, jnp.float32) * width * level
    return jnp.minimum(jnp.maximum(values, -reach), reach).astype(dtype)


def noise_with(key, extent, deviation, limit, cuts, heavy, kind=jnp.bfloat16):
    array = deviation * jax.random.normal(key, extent, jnp.float32)
    if cuts:
        array = array * shard_levels(key, extent, cuts, -0.22, 0.18)
    return jnp.clip(with_spikes(array, jax.random.fold_in(key, 3), *heavy), -limit, limit).astype(kind)


def setup_inputs(seed: int = 0) -> dict:
    key_list = jax.random.split(jax.random.key(seed), 7)
    return {
        "query_feats": noise_with(key_list[0], (QUERIES, D), 1.0, 24.0, ((0, 128),), (0, 1, 128, 5.5)),
        "key_feats": gaussian(key_list[1], (KEYS, D), 1.0, 6.0, ((0, 128),)),
        "key_task": with_ends(jax.random.randint(key_list[2], (KEYS,), 0, TASKS), jax.random.fold_in(key_list[2], 1), 0, TASKS - 1).astype(jnp.int32),
        "positive": with_ends(jax.random.randint(key_list[3], (QUERIES,), 0, KEYS), jax.random.fold_in(key_list[3], 1), 0, KEYS - 1).astype(jnp.int32),
        "head_weights": gaussian(key_list[4], (TASKS, D, E), D ** -0.5, 0.21875, ((2, 2),)),
        "task_scale": jnp.clip(jnp.exp(jax.random.uniform(key_list[5], (TASKS,), jnp.float32, math.log(10.0), math.log(30.0))), 10.0, 30.0),
    }


EPS = 1e-06

def grouped_project(rows, task, weights):
    count = rows.shape[0]
    block = math.gcd(count, 512)
    xs = rows.reshape(count // block, block, rows.shape[1])
    ts = task.reshape(count // block, block)

    def one_block(args):
        x, t = args
        out = jnp.zeros((block, weights.shape[2]), jnp.float32)
        for k in range(weights.shape[0]):
            proj = jnp.dot(x, weights[k], preferred_element_type=jnp.float32)
            out = jnp.where((t == k)[:, None], proj, out)
        return out
    return lax.map(one_block, (xs, ts)).reshape(count, weights.shape[2])

def grouped_grad(rows, task, grads, n_tasks):
    count = rows.shape[0]
    block = math.gcd(count, 512)
    xs = rows.reshape(count // block, block, rows.shape[1])
    gs = grads.reshape(count // block, block, grads.shape[1])
    ts = task.reshape(count // block, block)
    init = jnp.zeros((n_tasks, rows.shape[1], grads.shape[1]), jnp.float32)

    def step(total, args):
        x, g, t = args
        parts = []
        for k in range(n_tasks):
            masked = jnp.where((t == k)[:, None], g, jnp.zeros_like(g))
            parts.append(jnp.dot(x.T, masked, preferred_element_type=jnp.float32))
        return (total + jnp.stack(parts), None)
    total, unused = lax.scan(step, init, (xs, gs, ts))
    return total

def unit(proj):
    values = proj.astype(jnp.float32)
    inverse = 1.0 / jnp.sqrt(lax.optimization_barrier(jnp.sum(values * values, 1)) + EPS)
    return ((values * inverse[:, None]).astype(jnp.bfloat16), inverse)

def back(proj, inverse, grad):
    values = proj.astype(jnp.float32)
    inner = lax.optimization_barrier(jnp.sum(values * grad, 1))
    return (inverse[:, None] * grad - (inverse ** 3)[:, None] * values * inner[:, None]).astype(jnp.bfloat16)

def contrast(dots, scale_rows, task_rows, pos_rows, tasks_all):
    scores = dots * scale_rows[:, None]
    same = task_rows[:, None] == tasks_all[None, :]
    expo = jnp.exp(scores)
    expo = jnp.where(same, expo, jnp.zeros_like(expo))
    total = lax.optimization_barrier(jnp.sum(expo, 1))
    chosen = pos_rows[:, None] == lax.broadcasted_iota(jnp.int32, scores.shape, 1)
    loss = jnp.log(total) - lax.optimization_barrier(jnp.sum(jnp.where(chosen, scores, jnp.zeros_like(scores)), 1))
    target = jnp.where(chosen, jnp.ones_like(scores), jnp.zeros_like(scores))
    grads = (scale_rows[:, None] * (expo / total[:, None] - target)).astype(jnp.bfloat16)
    return (loss, grads)

def reference(query_feats, key_feats, key_task, positive, head_weights, task_scale):
    n_tasks = head_weights.shape[0]
    query_task = key_task[positive].astype(jnp.int32)
    query_proj = grouped_project(query_feats, query_task, head_weights).astype(jnp.bfloat16)
    key_proj = grouped_project(key_feats, key_task, head_weights).astype(jnp.bfloat16)
    query_unit, query_inv = unit(query_proj)
    key_unit, key_inv = unit(key_proj)
    query_scale = task_scale[query_task]
    count = query_feats.shape[0]
    block = math.gcd(count, 512)
    nb = count // block

    def step(key_total, args):
        q, s, t, p = args
        dots = jnp.dot(q, key_unit.T, preferred_element_type=jnp.float32)
        loss, grads = contrast(dots, s, t, p, key_task)
        query_back = jnp.dot(grads, key_unit, preferred_element_type=jnp.float32)
        key_total = key_total + jnp.dot(grads.T, q, preferred_element_type=jnp.float32)
        return (key_total, (loss, query_back))
    init = jnp.zeros(key_unit.shape, jnp.float32)
    key_back, (loss, query_back) = lax.scan(step, init, (query_unit.reshape(nb, block, -1), query_scale.reshape(nb, block), query_task.reshape(nb, block), positive.reshape(nb, block)))
    query_loss = loss.reshape(count)
    query_back = query_back.reshape(count, -1)
    query_grad = back(query_proj, query_inv, query_back)
    key_grad = back(key_proj, key_inv, key_back)
    weight_grad = grouped_grad(query_feats, query_task, query_grad, n_tasks) + grouped_grad(key_feats, key_task, key_grad, n_tasks)
    return (query_loss, weight_grad)
```

```python
import jax
import jax.numpy as jnp
from jax import lax
from jax.sharding import Mesh
from jax.sharding import PartitionSpec as P

FAR = ("dp_0", "dp_1", "dp_2")
CORE = "dp_3"
DP = FAR + (CORE,)
DP_TENSOR = DP + ("tensor",)
EPS = 1e-06
F32 = jnp.float32
BF16 = jnp.bfloat16


def swapped(x, axis):
    return lax.ppermute(x, axis, [(0, 1), (1, 0)])


def dot(a, b, dims):
    return lax.dot_general(a, b, (dims, ((), ())), preferred_element_type=F32)


def expansion(n_blocks, n_tasks, width, core, depth):
    rows = n_blocks * n_tasks * width
    row = lax.broadcasted_iota(jnp.int32, (rows, 1), 0)
    block, r = row // (n_tasks * width), row % width
    column = (2 * block + core) * width + r
    return (column == lax.broadcasted_iota(jnp.int32, (rows, depth), 1)).astype(BF16)


def by_task(rows, weights):
    return [dot(rows, weights[k], ((1,), (0,))).astype(BF16) for k in range(weights.shape[0])]


def chosen_task(parts, task):
    out = parts[0]
    for k in range(1, len(parts)):
        out = jnp.where((task == k)[:, None], parts[k], out)
    return out


def per_device(query_feats, key_feats, key_task, positive, head_weights, task_scale):
    core, member = lax.axis_index(CORE), lax.axis_index("tensor")
    n_tasks, depth, width = head_weights.shape
    n_query = query_feats.shape[0]
    own = n_query // 2
    n_far = lax.axis_size(FAR)
    per = key_feats.shape[0]
    out_rows = depth // (2 * n_far)

    feats = jnp.concatenate(
        [
            lax.dynamic_slice_in_dim(query_feats, member * own, own),
            lax.dynamic_slice_in_dim(query_feats, (1 - member) * own, own),
        ]
    )
    pos = jnp.concatenate(
        [
            lax.dynamic_slice_in_dim(positive, member * own, own),
            lax.dynamic_slice_in_dim(positive, (1 - member) * own, own),
        ]
    )

    tasks_in = jnp.broadcast_to(key_task.astype(BF16)[:, None], (per, 128))
    sent = jnp.concatenate([key_feats, tasks_in], 1)
    arrived = lax.all_to_all(
        jnp.broadcast_to(sent[None], (n_far, *sent.shape)), FAR, 0, 0, tiled=True
    ).reshape(n_far * per, depth + 128)
    keys = jnp.concatenate([arrived, swapped(arrived, CORE)])
    n_keys = keys.shape[0]
    at = lax.iota(jnp.int32, n_keys)
    half, inside = at // (n_far * per), at % (n_far * per)
    key_core = jnp.where(half == 0, core, 1 - core)
    key_index = (2 * (inside // per) + key_core) * per + inside % per
    all_feats, all_task = keys[:, :depth], keys[:, depth].astype(jnp.int32)

    chosen = pos[:, None] == key_index[None, :]
    query_task = jnp.sum(jnp.where(chosen, all_task[None, :], 0), 1)
    table = query_task[:own, None] == lax.broadcasted_iota(jnp.int32, (own, n_tasks), 1)
    scale = jnp.sum(jnp.where(table, task_scale[None, :], 0.0), 1)

    query_proj = chosen_task(by_task(feats, head_weights), query_task)
    key_proj = chosen_task(by_task(all_feats, head_weights), all_task)
    query_values, key_values = query_proj.astype(F32), key_proj.astype(F32)
    query_sq = jnp.sum(query_values * query_values, 1)
    key_sq = jnp.sum(key_values * key_values, 1)
    dots = dot(query_proj, key_proj, ((1,), (1,)))
    tail = jnp.concatenate(
        [
            key_sq[None, :],
            jnp.pad(query_sq, (0, n_keys - n_query))[None, :],
            jnp.zeros((6, n_keys), F32),
        ]
    )
    got = swapped(jnp.concatenate([dots[own:], tail]), "tensor")
    full = dots[:own] + got[:own]
    key_sq = key_sq + got[own]
    other_sq = got[own + 1, :n_query]
    query_sq = query_sq + jnp.concatenate([other_sq[own:], other_sq[:own]])
    query_inv = 1.0 / jnp.sqrt(query_sq + EPS)
    key_inv = 1.0 / jnp.sqrt(key_sq + EPS)

    half_cos = full * key_inv[None, :]
    scores = half_cos * (scale * query_inv[:own])[:, None]
    same = query_task[:own, None] == all_task[None, :]
    expo = jnp.where(same, jnp.exp(scores), 0.0)
    total = jnp.sum(expo, 1)
    target = chosen[:own]
    query_loss = jnp.log(total) - jnp.sum(jnp.where(target, scores, 0.0), 1)
    grads = (scale[:, None] * (expo / total[:, None] - target.astype(F32))).astype(BF16)
    wide = grads.astype(F32)
    query_inner = jnp.sum(wide * half_cos, 1)
    key_inner = jnp.sum(wide * full * query_inv[:own, None], 0)
    inner = jnp.stack([key_inner, jnp.pad(query_inner, (0, n_keys - own))])
    high = inner.astype(BF16)
    low = (inner - high.astype(F32)).astype(BF16)
    got = swapped(jnp.concatenate([grads, high, low, jnp.zeros((4, n_keys), BF16)]), "tensor")
    both = jnp.concatenate([grads, got[:own]])
    other = got[own : own + 2].astype(F32) + got[own + 2 : own + 4].astype(F32)
    key_inner = key_inner + other[0]
    query_inner = jnp.concatenate([query_inner, other[1, :own]])

    query_unit = (query_values * query_inv[:, None]).astype(BF16)
    key_unit = (key_values * key_inv[:, None]).astype(BF16)
    query_back = dot(both, key_unit, ((1,), (0,)))
    key_back = dot(both, query_unit, ((0,), (0,)))

    def through(values, inverse, back, inner):
        return (
            inverse[:, None] * back - (inverse**3)[:, None] * values * inner[:, None]
        ).astype(BF16)

    back = jnp.concatenate(
        [
            through(query_values, query_inv, query_back, query_inner),
            through(key_values, key_inv, key_back, key_inner),
        ]
    )

    row_feats = jnp.concatenate([feats, all_feats])
    row_task = jnp.concatenate([query_task, all_task])

    def share(of_core):
        spread = dot(
            expansion(n_far, n_tasks, out_rows, of_core, depth), row_feats, ((1,), (1,))
        ).astype(BF16)
        line_task = lax.iota(jnp.int32, spread.shape[0]) % (n_tasks * out_rows) // out_rows
        spread = jnp.where(line_task[:, None] == row_task[None, :], spread, jnp.zeros_like(spread))
        return dot(spread, back, ((1,), (0,)))

    away = share(1 - core).astype(BF16)
    mine = share(core) + swapped(away, CORE).astype(F32)
    blocks = mine.astype(BF16).reshape(n_far, n_tasks * out_rows, width)
    arrived = lax.all_to_all(blocks, FAR, 0, 0, tiled=True)
    weight_grad = jnp.sum(arrived.astype(F32), 0).reshape(n_tasks, out_rows, width)
    return (query_loss, weight_grad)


def solution(mesh):
    split = Mesh(
        mesh.devices.reshape(4, 2, 8, 2, mesh.shape["tensor"]),
        DP_TENSOR,
    )
    return jax.shard_map(
        per_device,
        mesh=split,
        in_specs=(P(DP, None), P(DP, None), P(DP), P(DP), P(None, None, "tensor"), P()),
        out_specs=(P(DP_TENSOR), P(None, DP, "tensor")),
        check_vma=False,
    )
```

```python
import jax
import jax.numpy as jnp
from jax import lax
from jax.sharding import Mesh
from jax.sharding import PartitionSpec as P

FAR = ("dp_0", "dp_1", "dp_2")
CORE = "dp_3"
DP = FAR + (CORE,)
DP_TENSOR = DP + ("tensor",)
EPS = 1e-06
F32 = jnp.float32
BF16 = jnp.bfloat16


def swapped(x, axis):
    return lax.ppermute(x, axis, [(0, 1), (1, 0)])


def dot(a, b, dims):
    return lax.dot_general(a, b, (dims, ((), ())), preferred_element_type=F32)


def expansion(n_blocks, n_tasks, width, core, depth):
    rows = n_blocks * n_tasks * width
    row = lax.broadcasted_iota(jnp.int32, (rows, 1), 0)
    block, r = row // (n_tasks * width), row % width
    column = (2 * block + core) * width + r
    return (column == lax.broadcasted_iota(jnp.int32, (rows, depth), 1)).astype(BF16)


def by_task(rows, weights):
    return [dot(rows, weights[k], ((1,), (0,))).astype(BF16) for k in range(weights.shape[0])]


def chosen_task(parts, task):
    out = parts[0]
    for k in range(1, len(parts)):
        out = jnp.where((task == k)[:, None], parts[k], out)
    return out


def per_device(query_feats, key_feats, key_task, positive, head_weights, task_scale):
    core, member = lax.axis_index(CORE), lax.axis_index("tensor")
    n_tasks, depth, width = head_weights.shape
    n_query = query_feats.shape[0]
    own = n_query // 2
    n_far = lax.axis_size(FAR)
    per = key_feats.shape[0]
    out_rows = depth // (2 * n_far)

    tasks_in = jnp.broadcast_to(key_task.astype(BF16)[:, None], (per, 128))
    sent = jnp.concatenate([key_feats, tasks_in], 1)
    sent, core, member = lax.optimization_barrier((sent, core, member))
    arrived = lax.all_to_all(
        jnp.broadcast_to(sent[None], (n_far, *sent.shape)), FAR, 0, 0, tiled=True
    ).reshape(n_far * per, depth + 128)
    arrived, query_feats, positive, core, member = lax.optimization_barrier(
        (arrived, query_feats, positive, core, member)
    )
    keys = jnp.concatenate([arrived, swapped(arrived, CORE)])

    feats = jnp.concatenate(
        [
            lax.dynamic_slice_in_dim(query_feats, member * own, own),
            lax.dynamic_slice_in_dim(query_feats, (1 - member) * own, own),
        ]
    )
    pos = jnp.concatenate(
        [
            lax.dynamic_slice_in_dim(positive, member * own, own),
            lax.dynamic_slice_in_dim(positive, (1 - member) * own, own),
        ]
    )

    n_keys = keys.shape[0]
    at = lax.iota(jnp.int32, n_keys)
    half, inside = at // (n_far * per), at % (n_far * per)
    key_core = jnp.where(half == 0, core, 1 - core)
    key_index = (2 * (inside // per) + key_core) * per + inside % per
    all_feats, all_task = keys[:, :depth], keys[:, depth].astype(jnp.int32)

    chosen = pos[:, None] == key_index[None, :]
    query_task = jnp.sum(jnp.where(chosen, all_task[None, :], 0), 1)
    table = query_task[:own, None] == lax.broadcasted_iota(jnp.int32, (own, n_tasks), 1)
    scale = jnp.sum(jnp.where(table, task_scale[None, :], 0.0), 1)

    row_feats = jnp.concatenate([feats, all_feats])
    row_task = jnp.concatenate([query_task, all_task])

    def spread(of_core):
        lines = dot(
            expansion(n_far, n_tasks, out_rows, of_core, depth), row_feats, ((1,), (1,))
        ).astype(BF16)
        line_task = lax.iota(jnp.int32, lines.shape[0]) % (n_tasks * out_rows) // out_rows
        return jnp.where(line_task[:, None] == row_task[None, :], lines, jnp.zeros_like(lines))

    away_feats, my_feats = lax.optimization_barrier((spread(1 - core), spread(core)))

    query_proj = chosen_task(by_task(feats, head_weights), query_task)
    key_proj = chosen_task(by_task(all_feats, head_weights), all_task)
    query_values, key_values = query_proj.astype(F32), key_proj.astype(F32)
    query_sq = jnp.sum(query_values * query_values, 1)
    key_sq = jnp.sum(key_values * key_values, 1)
    dots = dot(query_proj, key_proj, ((1,), (1,)))
    tail = jnp.stack([key_sq, jnp.tile(query_sq, n_keys // n_query)] * 4)
    got = swapped(jnp.concatenate([dots[own:], tail]), "tensor")
    full = dots[:own] + got[:own]
    key_sq = key_sq + got[own]
    other_sq = got[own + 1, :n_query]
    query_sq = query_sq + jnp.concatenate([other_sq[own:], other_sq[:own]])
    query_inv = 1.0 / jnp.sqrt(query_sq + EPS)
    key_inv = 1.0 / jnp.sqrt(key_sq + EPS)

    half_cos = full * key_inv[None, :]
    scores = half_cos * (scale * query_inv[:own])[:, None]
    same = query_task[:own, None] == all_task[None, :]
    expo = jnp.where(same, jnp.exp(scores), 0.0)
    total = jnp.sum(expo, 1)
    target = chosen[:own]
    query_loss = jnp.log(total) - jnp.sum(jnp.where(target, scores, 0.0), 1)
    grads = (scale[:, None] * (expo / total[:, None] - target.astype(F32))).astype(BF16)
    wide = grads.astype(F32)
    query_inner = jnp.sum(wide * half_cos, 1)
    key_inner = jnp.sum(wide * full * query_inv[:own, None], 0)
    inner = jnp.stack([key_inner, jnp.tile(query_inner, n_keys // own)])
    high = inner.astype(BF16)
    low = (inner - high.astype(F32)).astype(BF16)
    got = swapped(jnp.concatenate([grads, high, low, high, low]), "tensor")
    both = jnp.concatenate([grads, got[:own]])
    other = got[own : own + 2].astype(F32) + got[own + 2 : own + 4].astype(F32)
    key_inner = key_inner + other[0]
    query_inner = jnp.concatenate([query_inner, other[1, :own]])

    query_unit = (query_values * query_inv[:, None]).astype(BF16)
    key_unit = (key_values * key_inv[:, None]).astype(BF16)
    query_back = dot(both, key_unit, ((1,), (0,)))
    key_back = dot(both, query_unit, ((0,), (0,)))

    def through(values, inverse, back, inner):
        return (
            inverse[:, None] * back - (inverse**3)[:, None] * values * inner[:, None]
        ).astype(BF16)

    back = jnp.concatenate(
        [
            through(query_values, query_inv, query_back, query_inner),
            through(key_values, key_inv, key_back, key_inner),
        ]
    )

    away = dot(away_feats, back, ((1,), (0,))).astype(BF16)
    mine = lax.optimization_barrier(dot(my_feats, back, ((1,), (0,))))
    mine = mine + swapped(away, CORE).astype(F32)
    blocks = mine.astype(BF16).reshape(n_far, n_tasks * out_rows, width)
    blocks, query_loss = lax.optimization_barrier((blocks, query_loss))
    arrived = lax.all_to_all(blocks, FAR, 0, 0, tiled=True)
    weight_grad = jnp.sum(arrived.astype(F32), 0).reshape(n_tasks, out_rows, width)
    return (query_loss, weight_grad)


def solution(mesh):
    split = Mesh(
        mesh.devices.reshape(4, 2, 8, 2, mesh.shape["tensor"]),
        DP_TENSOR,
    )
    return jax.shard_map(
        per_device,
        mesh=split,
        in_specs=(P(DP, None), P(DP, None), P(DP), P(DP), P(None, None, "tensor"), P()),
        out_specs=(P(DP_TENSOR), P(None, DP, "tensor")),
        check_vma=False,
    )
```

```python
import functools

import jax
import jax.numpy as jnp
from jax import lax
from jax.experimental import pallas as pl
from jax.experimental.pallas import tpu as pltpu
from jax.sharding import Mesh
from jax.sharding import PartitionSpec as P

PLANE = ("dp_0", "dp_1")
LINE = "dp_2"
FAR = PLANE + (LINE,)
CORE = "dp_3"
DP = FAR + (CORE,)
DP_TENSOR = DP + ("tensor",)
EPS = 1e-06
F32 = jnp.float32
BF16 = jnp.bfloat16


def swapped(x, axis):
    return lax.ppermute(x, axis, [(0, 1), (1, 0)])


def dot(a, b, dims):
    return lax.dot_general(a, b, (dims, ((), ())), preferred_element_type=F32)


def lane_dense(column):
    eye = lax.broadcasted_iota(jnp.int32, (128, 128), 0) == lax.broadcasted_iota(
        jnp.int32, (128, 128), 1
    )
    return jnp.concatenate(
        [
            jnp.sum(jnp.where(eye, column[at : at + 128], 0.0), 0, keepdims=True)
            for at in range(0, column.shape[0], 128)
        ],
        1,
    )


def upright(line):
    eye = lax.broadcasted_iota(jnp.int32, (128, 128), 0) == lax.broadcasted_iota(
        jnp.int32, (128, 128), 1
    )
    return jnp.concatenate(
        [
            jnp.sum(jnp.where(eye, line[:, at : at + 128], 0.0), 1, keepdims=True)
            for at in range(0, line.shape[1], 128)
        ],
        0,
    )


def of_own_task(rows, task, weights):
    out = dot(rows, weights[0], ((1,), (0,)))
    for k in range(1, weights.shape[0]):
        out = jnp.where(task == k, dot(rows, weights[k], ((1,), (0,))), out)
    return out.astype(BF16)


def copies_kernel(x, out):
    rows = jnp.concatenate([x[k].astype(F32) for k in range(x.shape[0])]).astype(BF16)
    for k in range(out.shape[0]):
        out[k] = rows


def early_kernel(place, feats, mine, weights, rows, every_out, keys_out):
    depth, own = weights.shape[1], feats.shape[0] // 2
    for at, start in enumerate((place[1], 1 - place[1])):
        rows[at * own : (at + 1) * own] = feats[pl.ds(pl.multiple_of(start * own, own), own), :]
    keys_out[...] = of_own_task(mine[:, :depth], mine[:, depth : depth + 1].astype(F32), weights)
    for k in range(weights.shape[0]):
        every_out[k] = dot(rows[...], weights[k], ((1,), (0,))).astype(BF16)


def equal(a, b):
    return jnp.where(a == b, 1.0, 0.0)


def split(x):
    high = x.astype(BF16)
    rest = x - high.astype(F32)
    middle = rest.astype(BF16)
    return high, middle, (rest - middle.astype(F32)).astype(BF16)


def slots_of(slot, first, count):
    at = lax.broadcasted_iota(jnp.int32, (count, slot.shape[1]), 0) + first
    return equal(at.astype(F32), slot).astype(BF16)


def packed(dots, task, key_task, slot, first, count):
    pick = slots_of(slot, first, count)
    parts = split(jnp.where(task == key_task, dots, 0.0))
    high, middle, low = (dot(pick, part, ((1,), (1,))) for part in parts)
    out = (high + middle) + low
    half = out.shape[1] // 2
    return jnp.concatenate([out[:, half:], out[:, :half]], 1)


def unpacked(slots, slot, first):
    pick = slots_of(slot, first, slots.shape[0])
    high, middle, low = (dot(part, pick, ((0,), (0,))) for part in split(slots))
    return (high + middle) + low


def index_of_keys(place, per, n_keys):
    half = n_keys // 2
    at = lax.broadcasted_iota(jnp.int32, (1, n_keys), 1)
    inside = lax.rem(at, half)
    key_core = jnp.where(at < half, place[0], 1 - place[0])
    return ((2 * lax.div(inside, per) + key_core) * per + lax.rem(inside, per)).astype(F32)


def late_kernel(
    per, place, positive, mine, theirs, mine_proj, every, weights,
    dots_out, message, query_out, keys_out, columns, lines, count_out,
):
    depth, n_query = weights.shape[1], dots_out.shape[0]
    half, own = mine.shape[0], n_query // 2
    keys_out[:half] = mine_proj[...]
    keys_out[half:] = of_own_task(
        theirs[:, :depth], theirs[:, depth : depth + 1].astype(F32), weights
    )
    upright_task = jnp.concatenate(
        [mine[:, depth : depth + 1].astype(F32), theirs[:, depth : depth + 1].astype(F32)]
    )
    key_task = jnp.concatenate(
        [lane_dense(mine[:, depth:].astype(F32)), lane_dense(theirs[:, depth:].astype(F32))], 1
    )
    before = lax.broadcasted_iota(jnp.int32, (2 * half, 2 * half), 0) < lax.broadcasted_iota(
        jnp.int32, (2 * half, 2 * half), 1
    )
    slot = jnp.sum(
        jnp.where(before, equal(upright_task, key_task), 0.0), 0, keepdims=True
    )
    count_out[0] = (jnp.max(slot) + 1.0).astype(jnp.int32)
    line = positive[...].astype(F32)
    pos = upright(
        jnp.where(place[1] == 0, line, jnp.concatenate([line[:, own:], line[:, :own]], 1))
    )
    chosen = pos == index_of_keys(place, per, 2 * half)
    task = jnp.sum(jnp.where(chosen, key_task, 0.0), 1, keepdims=True)
    first = lax.broadcasted_iota(jnp.int32, columns.shape, 1) == 0
    columns[...] = jnp.where(first, task, pos)
    query = every[0].astype(F32)
    for k in range(1, weights.shape[0]):
        query = jnp.where(task == k, every[k].astype(F32), query)
    query_out[...] = query.astype(BF16)
    keys = keys_out[...]
    wide = keys.astype(F32)
    query_sq = lane_dense(jnp.sum(query * query, 1, keepdims=True))
    key_sq = lane_dense(jnp.sum(wide * wide, 1, keepdims=True))
    dots = dot(query_out[...], keys, ((1,), (1,)))
    dots_out[...] = dots
    at = lax.broadcasted_iota(jnp.int32, lines.shape, 0)
    lines[...] = jnp.where(
        at == 0,
        jnp.concatenate([lane_dense(task), key_task], 1),
        jnp.where(
            at == 1,
            jnp.concatenate([query_sq, slot], 1),
            jnp.concatenate([query_sq, key_sq], 1),
        ),
    )
    n_slots = message.shape[0] - 8
    message[:n_slots] = packed(dots, task, key_task, slot, 0, n_slots)
    at = lax.broadcasted_iota(jnp.int32, (8, n_query), 0)
    swapped_sq = jnp.concatenate([query_sq[:, own:], query_sq[:, :own]], 1)
    message[n_slots:] = jnp.where(
        at == 0, swapped_sq, jnp.where(at == 1, key_sq[:, :half], key_sq[:, half:])
    )


def overflow_kernel(n_slots, dots, columns, lines, out):
    n_query = dots.shape[0]
    out[...] = packed(
        dots[...],
        columns[:, :1],
        lines[0:1, n_query:],
        lines[1:2, n_query:],
        n_slots,
        out.shape[0],
    )


def contrast_kernel(
    per, place, count, task_scale, dots, got, over, columns, lines, query_proj, key_proj,
    loss_out, back, full,
):
    n_query, n_keys = dots.shape
    own, n_slots = n_query // 2, got.shape[0] - 8
    task, pos = columns[:, :1], columns[:, 1:2]
    key_task, slot = lines[0:1, n_query:], lines[1:2, n_query:]
    full[...] = dots[...] + unpacked(got[:n_slots], slot, 0)

    @pl.when(count[0] > n_slots)
    def _():
        full[...] += unpacked(over[...], slot, n_slots)

    query_sq = lines[1:2, :n_query] + got[n_slots : n_slots + 1]
    key_sq = lines[2:3, n_query:] + jnp.concatenate(
        [got[n_slots + 1 : n_slots + 2], got[n_slots + 2 : n_slots + 3]], 1
    )
    key_line = 1.0 / jnp.sqrt(key_sq + EPS)
    query_inv, key_inv = upright(1.0 / jnp.sqrt(query_sq + EPS)), upright(key_line)
    scale = jnp.full(task.shape, task_scale[0], F32)
    for k in range(1, task_scale.shape[0]):
        scale = jnp.where(task == k, task_scale[k], scale)
    whole = full[...]
    half_cos = whole * key_line
    scores = half_cos * (scale * query_inv)
    expo = jnp.where(task == key_task, jnp.exp(scores), 0.0)
    chosen = pos == index_of_keys(place, per, n_keys)
    total = jnp.sum(expo, 1, keepdims=True)
    picked = jnp.sum(jnp.where(chosen, scores, 0.0), 1, keepdims=True)
    loss_out[...] = lane_dense((jnp.log(total) - picked)[:own])
    grads = scale * (expo * (1.0 / total) - jnp.where(chosen, 1.0, 0.0))
    grads = grads.astype(BF16)
    wide = grads.astype(F32)
    query_inner = jnp.sum(wide * half_cos, 1, keepdims=True)
    key_inner = upright(jnp.sum(wide * whole * query_inv, 0, keepdims=True))
    query_values, key_values = query_proj[...].astype(F32), key_proj[...].astype(F32)
    query_back = dot(grads, (key_values * key_inv).astype(BF16), ((1,), (0,)))
    key_back = dot(grads, (query_values * query_inv).astype(BF16), ((0,), (0,)))

    def through(values, inverse, grad, inner):
        return (inverse * grad - (inverse * inverse * inverse * inner) * values).astype(BF16)

    back[:n_query] = through(query_values, query_inv, query_back, query_inner)
    back[n_query:] = through(key_values, key_inv, key_back, key_inner)


def spread_kernel(width, n_tasks, place, rows, mine, theirs, task, away, here):
    depth = rows.shape[1]
    half, lines = depth // 2, away.shape[0] // 2
    line = lax.broadcasted_iota(jnp.int32, (lines, 1), 0)
    block = lax.div(line, n_tasks * width)
    r = lax.div(lax.rem(line, n_tasks * width), n_tasks)
    line_task = lax.rem(line, n_tasks).astype(F32)
    same = line_task == task[:1, :]
    for out, core in ((away, 1 - place[0]), (here, place[0])):
        column = (2 * block + core) * width + r
        pick = (column == lax.broadcasted_iota(jnp.int32, (lines, half), 1)).astype(F32).astype(BF16)
        for h in range(2):
            at = 0
            for part in (rows, mine, theirs):
                n = part.shape[0]
                got = dot(pick, part[:, h * half : (h + 1) * half], ((1,), (1,)))
                got = jnp.where(same[:, at : at + n], got, 0.0)
                out[h * lines : (h + 1) * lines, at : at + n] = got.astype(BF16)
                at += n


def in_vmem(n):
    return [pl.BlockSpec(memory_space=pltpu.SMEM)] + [pl.BlockSpec(memory_space=pltpu.VMEM)] * n


SLOTS = 176
ROOM = pltpu.CompilerParams(vmem_limit_bytes=16 << 20)


def cost(flops, moved):
    return pl.CostEstimate(flops=flops, bytes_accessed=moved, transcendentals=0)


def per_device(query_feats, key_feats, key_task, positive, head_weights, task_scale):
    core, member = lax.axis_index(CORE), lax.axis_index("tensor")
    n_tasks, depth, width = head_weights.shape
    n_query = query_feats.shape[0]
    own = n_query // 2
    n_far = lax.axis_size(FAR)
    per = key_feats.shape[0]
    out_rows = depth // (2 * n_far)

    tasks_in = jnp.broadcast_to(key_task.astype(BF16)[:, None], (per, 128))
    sent = jnp.concatenate([key_feats, tasks_in], 1)
    sent = jnp.broadcast_to(sent[None], (lax.axis_size(LINE), *sent.shape))
    place = jnp.stack([core, member])
    sent, place, positive = lax.optimization_barrier((sent, place, positive[None]))
    sent = lax.all_to_all(sent, LINE, 0, 0, tiled=True)
    sent = pl.pallas_call(
        copies_kernel,
        out_shape=jax.ShapeDtypeStruct(
            (lax.axis_size(PLANE), sent.shape[0] * per, depth + 128), BF16
        ),
        in_specs=in_vmem(1)[1:],
        out_specs=in_vmem(1)[1],
        compiler_params=ROOM,
        cost_estimate=cost(1 << 33, 1 << 20),
    )(sent)
    sent = lax.all_to_all(sent, PLANE, 0, 0, tiled=True).reshape(-1, depth + 128)
    arrived = sent
    arrived, place, positive = lax.optimization_barrier((arrived, place, positive))
    theirs = swapped(arrived, CORE)
    n_half = n_far * per
    n_keys = 2 * n_half

    feats, every, mine_proj = pl.pallas_call(
        early_kernel,
        out_shape=(
            jax.ShapeDtypeStruct((n_query, depth), BF16),
            jax.ShapeDtypeStruct((n_tasks, n_query, width), BF16),
            jax.ShapeDtypeStruct((n_half, width), BF16),
        ),
        in_specs=in_vmem(3),
        compiler_params=ROOM,
        out_specs=tuple(in_vmem(3)[1:]),
        cost_estimate=cost(2 * n_tasks * (n_query + n_half) * depth * width, 6 << 20),
    )(place, query_feats, arrived, head_weights)
    dots, message, query_proj, key_proj, columns, lines, count = pl.pallas_call(
        functools.partial(late_kernel, per),
        out_shape=(
            jax.ShapeDtypeStruct((n_query, n_keys), F32),
            jax.ShapeDtypeStruct((SLOTS + 8, n_query), F32),
            jax.ShapeDtypeStruct((n_query, width), BF16),
            jax.ShapeDtypeStruct((n_keys, width), BF16),
            jax.ShapeDtypeStruct((n_query, 128), F32),
            jax.ShapeDtypeStruct((8, n_query + n_keys), F32),
            jax.ShapeDtypeStruct((1,), jnp.int32),
        ),
        in_specs=in_vmem(6),
        out_specs=tuple(in_vmem(6)[1:] + in_vmem(0)),
        compiler_params=ROOM,
        cost_estimate=cost(2 * n_tasks * n_half * depth * width, 6 << 20),
    )(place, positive, arrived, theirs, mine_proj, every, head_weights)
    got = swapped(message, "tensor")

    def follow(operands):
        rest = pl.pallas_call(
            functools.partial(overflow_kernel, SLOTS),
            out_shape=jax.ShapeDtypeStruct((n_keys - SLOTS, n_query), F32),
            in_specs=in_vmem(3)[1:],
            out_specs=in_vmem(1)[1],
            compiler_params=ROOM,
        )(*operands)
        return swapped(rest, "tensor")

    def nothing(operands):
        return jnp.zeros((n_keys - SLOTS, n_query), F32)

    over = lax.cond(count[0] > SLOTS, follow, nothing, (dots, columns, lines))

    n_lines = n_far * n_tasks * out_rows
    away_feats, my_feats = pl.pallas_call(
        functools.partial(spread_kernel, out_rows, n_tasks),
        out_shape=(jax.ShapeDtypeStruct((n_lines, n_query + n_keys), BF16),) * 2,
        in_specs=in_vmem(4),
        out_specs=tuple(in_vmem(2)[1:]),
        compiler_params=ROOM,
        cost_estimate=cost(2 * n_lines * (n_query + n_keys) * depth, 6 << 20),
    )(place, feats, arrived, theirs, lines)
    query_loss, back = pl.pallas_call(
        functools.partial(contrast_kernel, per),
        out_shape=(
            jax.ShapeDtypeStruct((1, own), F32),
            jax.ShapeDtypeStruct((n_query + n_keys, width), BF16),
        ),
        in_specs=in_vmem(0) * 3 + in_vmem(7)[1:],
        out_specs=tuple(in_vmem(2)[1:]),
        scratch_shapes=[pltpu.VMEM((n_query, n_keys), F32)],
        compiler_params=ROOM,
        cost_estimate=cost(20 * n_query * n_keys * width, 6 << 20),
    )(place, count, task_scale, dots, got, over, columns, lines, query_proj, key_proj)
    query_loss = query_loss.reshape(own)

    away = dot(away_feats, back, ((1,), (0,))).astype(BF16)
    mine = lax.optimization_barrier(dot(my_feats, back, ((1,), (0,))))
    mine = mine + swapped(away, CORE).astype(F32)
    n_plane, n_line = lax.axis_size(PLANE), lax.axis_size(LINE)
    blocks = mine.astype(BF16).reshape(n_plane, -1, width)
    blocks, query_loss = lax.optimization_barrier((blocks, query_loss))
    arrived = lax.all_to_all(blocks, PLANE, 0, 0, tiled=True)
    blocks = sum(arrived[k].astype(F32) for k in range(n_plane))
    blocks = blocks.astype(BF16).reshape(n_line, -1, width)
    arrived = lax.all_to_all(blocks, LINE, 0, 0, tiled=True)
    weight_grad = jnp.sum(arrived.astype(F32), 0).reshape(out_rows, n_tasks, width)
    weight_grad = weight_grad.transpose(1, 0, 2)
    return (query_loss, weight_grad)


def solution(mesh):
    split = Mesh(
        mesh.devices.reshape(4, 2, 8, 2, mesh.shape["tensor"]),
        DP_TENSOR,
    )
    return jax.shard_map(
        per_device,
        mesh=split,
        in_specs=(P(DP, None), P(DP, None), P(DP), P(DP), P(None, None, "tensor"), P()),
        out_specs=(P(DP_TENSOR), P(None, DP, "tensor")),
        check_vma=False,
    )
```

```python
import functools

import jax
import jax.numpy as jnp
from jax import lax
from jax.experimental import pallas as pl
from jax.experimental.pallas import tpu as pltpu
from jax.sharding import Mesh
from jax.sharding import PartitionSpec as P

PLANE = ("dp_0", "dp_1")
LINE = "dp_2"
FAR = PLANE + (LINE,)
CORE = "dp_3"
DP = FAR + (CORE,)
DP_TENSOR = DP + ("tensor",)
EPS = 1e-06
F32 = jnp.float32
BF16 = jnp.bfloat16


def swapped(x, axis):
    return lax.ppermute(x, axis, [(0, 1), (1, 0)])


def dot(a, b, dims):
    return lax.dot_general(a, b, (dims, ((), ())), preferred_element_type=F32)


def lane_dense(column):
    eye = lax.broadcasted_iota(jnp.int32, (128, 128), 0) == lax.broadcasted_iota(
        jnp.int32, (128, 128), 1
    )
    return jnp.concatenate(
        [
            jnp.sum(jnp.where(eye, column[at : at + 128], 0.0), 0, keepdims=True)
            for at in range(0, column.shape[0], 128)
        ],
        1,
    )


def upright(line):
    eye = lax.broadcasted_iota(jnp.int32, (128, 128), 0) == lax.broadcasted_iota(
        jnp.int32, (128, 128), 1
    )
    return jnp.concatenate(
        [
            jnp.sum(jnp.where(eye, line[:, at : at + 128], 0.0), 1, keepdims=True)
            for at in range(0, line.shape[1], 128)
        ],
        0,
    )


def of_own_task(rows, task, weights):
    out = dot(rows, weights[0], ((1,), (0,)))
    for k in range(1, weights.shape[0]):
        out = jnp.where(task == k, dot(rows, weights[k], ((1,), (0,))), out)
    return out.astype(BF16)


def task_kernel(task, out):
    row = lax.broadcasted_iota(jnp.int32, out.shape, 0)
    tasks = jnp.full(out.shape, task[0], jnp.int32)
    for k in range(1, out.shape[0]):
        tasks = jnp.where(row == k, task[k], tasks)
    out[...] = tasks.astype(F32).astype(BF16)


def copies_kernel(x, out):
    rows = jnp.concatenate([x[k].astype(F32) for k in range(x.shape[0])]).astype(BF16)
    for k in range(out.shape[0]):
        out[k] = rows


def early_kernel(place, feats, mine, weights, rows, every_out, keys_out):
    depth, own = weights.shape[1], feats.shape[0] // 2
    for at, start in enumerate((place[1], 1 - place[1])):
        rows[at * own : (at + 1) * own] = feats[pl.ds(pl.multiple_of(start * own, own), own), :]
    keys_out[...] = of_own_task(mine[:, :depth], mine[:, depth : depth + 1].astype(F32), weights)
    for k in range(weights.shape[0]):
        every_out[k] = dot(rows[...], weights[k], ((1,), (0,))).astype(BF16)


def equal(a, b):
    return jnp.where(a == b, 1.0, 0.0)


def split(x):
    high = x.astype(BF16)
    rest = x - high.astype(F32)
    middle = rest.astype(BF16)
    return high, middle, (rest - middle.astype(F32)).astype(BF16)


def slots_of(slot, first, count):
    at = lax.broadcasted_iota(jnp.int32, (count, slot.shape[1]), 0) + first
    return equal(at.astype(F32), slot).astype(BF16)


def packed(dots, task, key_task, slot, first, count):
    pick = slots_of(slot, first, count)
    parts = split(jnp.where(task == key_task, dots, 0.0))
    high, middle, low = (dot(pick, part, ((1,), (1,))) for part in parts)
    out = (high + middle) + low
    half = out.shape[1] // 2
    return jnp.concatenate([out[:, half:], out[:, :half]], 1)


def unpacked(slots, slot, first):
    pick = slots_of(slot, first, slots.shape[0])
    high, middle, low = (dot(part, pick, ((0,), (0,))) for part in split(slots))
    return (high + middle) + low


def index_of_keys(place, per, n_keys):
    half = n_keys // 2
    at = lax.broadcasted_iota(jnp.int32, (1, n_keys), 1)
    inside = lax.rem(at, half)
    key_core = jnp.where(at < half, place[0], 1 - place[0])
    return ((2 * lax.div(inside, per) + key_core) * per + lax.rem(inside, per)).astype(F32)


def late_kernel(
    per, place, positive, mine, theirs, mine_proj, every, weights,
    dots_out, message, query_out, keys_out, columns, lines, count_out,
):
    depth, n_query = weights.shape[1], dots_out.shape[0]
    half, own = mine.shape[0], n_query // 2
    keys_out[:half] = mine_proj[...]
    keys_out[half:] = of_own_task(
        theirs[:, :depth], theirs[:, depth : depth + 1].astype(F32), weights
    )
    upright_task = jnp.concatenate(
        [mine[:, depth : depth + 1].astype(F32), theirs[:, depth : depth + 1].astype(F32)]
    )
    key_task = jnp.concatenate(
        [lane_dense(mine[:, depth:].astype(F32)), lane_dense(theirs[:, depth:].astype(F32))], 1
    )
    before = lax.broadcasted_iota(jnp.int32, (2 * half, 2 * half), 0) < lax.broadcasted_iota(
        jnp.int32, (2 * half, 2 * half), 1
    )
    slot = jnp.sum(
        jnp.where(before, equal(upright_task, key_task), 0.0), 0, keepdims=True
    )
    count_out[0] = (jnp.max(slot) + 1.0).astype(jnp.int32)
    line = positive[...].astype(F32)
    pos = upright(
        jnp.where(place[1] == 0, line, jnp.concatenate([line[:, own:], line[:, :own]], 1))
    )
    chosen = pos == index_of_keys(place, per, 2 * half)
    task = jnp.sum(jnp.where(chosen, key_task, 0.0), 1, keepdims=True)
    first = lax.broadcasted_iota(jnp.int32, columns.shape, 1) == 0
    columns[...] = jnp.where(first, task, pos)
    query = every[0].astype(F32)
    for k in range(1, weights.shape[0]):
        query = jnp.where(task == k, every[k].astype(F32), query)
    query_out[...] = query.astype(BF16)
    keys = keys_out[...]
    wide = keys.astype(F32)
    query_sq = lane_dense(jnp.sum(query * query, 1, keepdims=True))
    key_sq = lane_dense(jnp.sum(wide * wide, 1, keepdims=True))
    dots = dot(query_out[...], keys, ((1,), (1,)))
    dots_out[...] = dots
    at = lax.broadcasted_iota(jnp.int32, lines.shape, 0)
    lines[...] = jnp.where(
        at == 0,
        jnp.concatenate([lane_dense(task), key_task], 1),
        jnp.where(
            at == 1,
            jnp.concatenate([query_sq, slot], 1),
            jnp.concatenate([query_sq, key_sq], 1),
        ),
    )
    n_slots = message.shape[0] - 8
    message[:n_slots] = packed(dots, task, key_task, slot, 0, n_slots)
    at = lax.broadcasted_iota(jnp.int32, (8, n_query), 0)
    swapped_sq = jnp.concatenate([query_sq[:, own:], query_sq[:, :own]], 1)
    message[n_slots:] = jnp.where(
        at == 0, swapped_sq, jnp.where(at == 1, key_sq[:, :half], key_sq[:, half:])
    )


def overflow_kernel(n_slots, dots, columns, lines, out):
    n_query = dots.shape[0]
    out[...] = packed(
        dots[...],
        columns[:, :1],
        lines[0:1, n_query:],
        lines[1:2, n_query:],
        n_slots,
        out.shape[0],
    )


def contrast_kernel(
    per, place, count, task_scale, dots, got, over, columns, lines, query_proj, key_proj,
    loss_out, back, full,
):
    n_query, n_keys = dots.shape
    own, n_slots = n_query // 2, got.shape[0] - 8
    task, pos = columns[:, :1], columns[:, 1:2]
    key_task, slot = lines[0:1, n_query:], lines[1:2, n_query:]
    full[...] = dots[...] + unpacked(got[:n_slots], slot, 0)

    @pl.when(count[0] > n_slots)
    def _():
        full[...] += unpacked(over[...], slot, n_slots)

    query_sq = lines[1:2, :n_query] + got[n_slots : n_slots + 1]
    key_sq = lines[2:3, n_query:] + jnp.concatenate(
        [got[n_slots + 1 : n_slots + 2], got[n_slots + 2 : n_slots + 3]], 1
    )
    key_line = 1.0 / jnp.sqrt(key_sq + EPS)
    query_inv, key_inv = upright(1.0 / jnp.sqrt(query_sq + EPS)), upright(key_line)
    scale = jnp.full(task.shape, task_scale[0], F32)
    for k in range(1, task_scale.shape[0]):
        scale = jnp.where(task == k, task_scale[k], scale)
    whole = full[...]
    half_cos = whole * key_line
    scores = half_cos * (scale * query_inv)
    expo = jnp.where(task == key_task, jnp.exp(scores), 0.0)
    chosen = pos == index_of_keys(place, per, n_keys)
    total = jnp.sum(expo, 1, keepdims=True)
    picked = jnp.sum(jnp.where(chosen, scores, 0.0), 1, keepdims=True)
    loss_out[...] = lane_dense((jnp.log(total) - picked)[:own])
    grads = scale * (expo * (1.0 / total) - jnp.where(chosen, 1.0, 0.0))
    grads = grads.astype(BF16)
    wide = grads.astype(F32)
    query_inner = jnp.sum(wide * half_cos, 1, keepdims=True)
    key_inner = upright(jnp.sum(wide * whole * query_inv, 0, keepdims=True))
    query_values, key_values = query_proj[...].astype(F32), key_proj[...].astype(F32)
    query_back = dot(grads, (key_values * key_inv).astype(BF16), ((1,), (0,)))
    key_back = dot(grads, (query_values * query_inv).astype(BF16), ((0,), (0,)))

    def through(values, inverse, grad, inner):
        return (inverse * grad - (inverse * inverse * inverse * inner) * values).astype(BF16)

    back[:n_query] = through(query_values, query_inv, query_back, query_inner)
    back[n_query:] = through(key_values, key_inv, key_back, key_inner)


def spread_kernel(width, n_tasks, place, rows, mine, theirs, task, away, here):
    depth = rows.shape[1]
    half, lines = depth // 2, away.shape[0] // 2
    line = lax.broadcasted_iota(jnp.int32, (lines, 1), 0)
    block = lax.div(line, n_tasks * width)
    r = lax.div(lax.rem(line, n_tasks * width), n_tasks)
    line_task = lax.rem(line, n_tasks).astype(F32)
    same = line_task == task[:1, :]
    for out, core in ((away, 1 - place[0]), (here, place[0])):
        column = (2 * block + core) * width + r
        pick = (column == lax.broadcasted_iota(jnp.int32, (lines, half), 1)).astype(F32).astype(BF16)
        for h in range(2):
            at = 0
            for part in (rows, mine, theirs):
                n = part.shape[0]
                got = dot(pick, part[:, h * half : (h + 1) * half], ((1,), (1,)))
                got = jnp.where(same[:, at : at + n], got, 0.0)
                out[h * lines : (h + 1) * lines, at : at + n] = got.astype(BF16)
                at += n


def in_vmem(n):
    return [pl.BlockSpec(memory_space=pltpu.SMEM)] + [pl.BlockSpec(memory_space=pltpu.VMEM)] * n


SLOTS = 160
ROOM = pltpu.CompilerParams(vmem_limit_bytes=16 << 20)


def cost(flops, moved):
    return pl.CostEstimate(flops=flops, bytes_accessed=moved, transcendentals=0)


def per_device(query_feats, key_feats, key_task, positive, head_weights, task_scale):
    core, member = lax.axis_index(CORE), lax.axis_index("tensor")
    n_tasks, depth, width = head_weights.shape
    n_query = query_feats.shape[0]
    own = n_query // 2
    n_far = lax.axis_size(FAR)
    per = key_feats.shape[0]
    out_rows = depth // (2 * n_far)

    tasks_in = pl.pallas_call(
        task_kernel,
        out_shape=jax.ShapeDtypeStruct((per, 128), BF16),
        in_specs=in_vmem(0),
        out_specs=in_vmem(1)[1],
        compiler_params=ROOM,
        cost_estimate=cost(1 << 30, 1 << 12),
    )(key_task)
    sent = jnp.concatenate([key_feats, tasks_in], 1)
    sent = jnp.broadcast_to(sent[None], (lax.axis_size(LINE), *sent.shape))
    place = jnp.stack([core, member])
    sent, place, positive = lax.optimization_barrier((sent, place, positive[None]))
    sent = lax.all_to_all(sent, LINE, 0, 0, tiled=True)
    sent = pl.pallas_call(
        copies_kernel,
        out_shape=jax.ShapeDtypeStruct(
            (lax.axis_size(PLANE), sent.shape[0] * per, depth + 128), BF16
        ),
        in_specs=in_vmem(1)[1:],
        out_specs=in_vmem(1)[1],
        compiler_params=ROOM,
        cost_estimate=cost(1 << 33, 1 << 20),
    )(sent)
    sent = lax.all_to_all(sent, PLANE, 0, 0, tiled=True).reshape(-1, depth + 128)
    arrived = sent
    arrived, place, positive = lax.optimization_barrier((arrived, place, positive))
    theirs = swapped(arrived, CORE)
    n_half = n_far * per
    n_keys = 2 * n_half

    feats, every, mine_proj = pl.pallas_call(
        early_kernel,
        out_shape=(
            jax.ShapeDtypeStruct((n_query, depth), BF16),
            jax.ShapeDtypeStruct((n_tasks, n_query, width), BF16),
            jax.ShapeDtypeStruct((n_half, width), BF16),
        ),
        in_specs=in_vmem(3),
        compiler_params=ROOM,
        out_specs=tuple(in_vmem(3)[1:]),
        cost_estimate=cost(2 * n_tasks * (n_query + n_half) * depth * width, 6 << 20),
    )(place, query_feats, arrived, head_weights)
    dots, message, query_proj, key_proj, columns, lines, count = pl.pallas_call(
        functools.partial(late_kernel, per),
        out_shape=(
            jax.ShapeDtypeStruct((n_query, n_keys), F32),
            jax.ShapeDtypeStruct((SLOTS + 8, n_query), F32),
            jax.ShapeDtypeStruct((n_query, width), BF16),
            jax.ShapeDtypeStruct((n_keys, width), BF16),
            jax.ShapeDtypeStruct((n_query, 128), F32),
            jax.ShapeDtypeStruct((8, n_query + n_keys), F32),
            jax.ShapeDtypeStruct((1,), jnp.int32),
        ),
        in_specs=in_vmem(6),
        out_specs=tuple(in_vmem(6)[1:] + in_vmem(0)),
        compiler_params=ROOM,
        cost_estimate=cost(2 * n_tasks * n_half * depth * width, 6 << 20),
    )(place, positive, arrived, theirs, mine_proj, every, head_weights)
    got = swapped(message, "tensor")

    def follow(operands):
        rest = pl.pallas_call(
            functools.partial(overflow_kernel, SLOTS),
            out_shape=jax.ShapeDtypeStruct((n_keys - SLOTS, n_query), F32),
            in_specs=in_vmem(3)[1:],
            out_specs=in_vmem(1)[1],
            compiler_params=ROOM,
        )(*operands)
        return swapped(rest, "tensor")

    def nothing(operands):
        return jnp.zeros((n_keys - SLOTS, n_query), F32)

    over = lax.cond(count[0] > SLOTS, follow, nothing, (dots, columns, lines))

    n_lines = n_far * n_tasks * out_rows
    away_feats, my_feats = pl.pallas_call(
        functools.partial(spread_kernel, out_rows, n_tasks),
        out_shape=(jax.ShapeDtypeStruct((n_lines, n_query + n_keys), BF16),) * 2,
        in_specs=in_vmem(4),
        out_specs=tuple(in_vmem(2)[1:]),
        compiler_params=ROOM,
        cost_estimate=cost(2 * n_lines * (n_query + n_keys) * depth, 6 << 20),
    )(place, feats, arrived, theirs, lines)
    query_loss, back = pl.pallas_call(
        functools.partial(contrast_kernel, per),
        out_shape=(
            jax.ShapeDtypeStruct((1, own), F32),
            jax.ShapeDtypeStruct((n_query + n_keys, width), BF16),
        ),
        in_specs=in_vmem(0) * 3 + in_vmem(7)[1:],
        out_specs=tuple(in_vmem(2)[1:]),
        scratch_shapes=[pltpu.VMEM((n_query, n_keys), F32)],
        compiler_params=ROOM,
        cost_estimate=cost(20 * n_query * n_keys * width, 6 << 20),
    )(place, count, task_scale, dots, got, over, columns, lines, query_proj, key_proj)
    query_loss = query_loss.reshape(own)

    away = dot(away_feats, back, ((1,), (0,))).astype(BF16)
    mine = lax.optimization_barrier(dot(my_feats, back, ((1,), (0,))))
    mine = mine + swapped(away, CORE).astype(F32)
    n_plane, n_line = lax.axis_size(PLANE), lax.axis_size(LINE)
    blocks = mine.astype(BF16).reshape(n_plane, -1, width)
    blocks, query_loss = lax.optimization_barrier((blocks, query_loss))
    arrived = lax.all_to_all(blocks, PLANE, 0, 0, tiled=True)
    blocks = sum(arrived[k].astype(F32) for k in range(n_plane))
    blocks = blocks.astype(BF16).reshape(n_line, -1, width)
    arrived = lax.all_to_all(blocks, LINE, 0, 0, tiled=True)
    weight_grad = jnp.sum(arrived.astype(F32), 0).reshape(out_rows, n_tasks, width)
    weight_grad = weight_grad.transpose(1, 0, 2)
    return (query_loss, weight_grad)


def solution(mesh):
    split = Mesh(
        mesh.devices.reshape(4, 2, 8, 2, mesh.shape["tensor"]),
        DP_TENSOR,
    )
    return jax.shard_map(
        per_device,
        mesh=split,
        in_specs=(P(DP, None), P(DP, None), P(DP), P(DP), P(None, None, "tensor"), P()),
        out_specs=(P(DP_TENSOR), P(None, DP, "tensor")),
        check_vma=False,
    )
```

```python
import functools

import jax
import jax.numpy as jnp
from jax import lax
from jax.experimental import pallas as pl
from jax.experimental.pallas import tpu as pltpu
from jax.sharding import Mesh
from jax.sharding import PartitionSpec as P

PLANE = ("dp_0", "dp_1")
LINE = "dp_2"
FAR = PLANE + (LINE,)
CORE = "dp_3"
DP = FAR + (CORE,)
DP_TENSOR = DP + ("tensor",)
EPS = 1e-06
F32 = jnp.float32
BF16 = jnp.bfloat16


def swapped(x, axis):
    return lax.ppermute(x, axis, [(0, 1), (1, 0)])


def dot(a, b, dims):
    return lax.dot_general(a, b, (dims, ((), ())), preferred_element_type=F32)


def lane_dense(column):
    eye = lax.broadcasted_iota(jnp.int32, (128, 128), 0) == lax.broadcasted_iota(
        jnp.int32, (128, 128), 1
    )
    return jnp.concatenate(
        [
            jnp.sum(jnp.where(eye, column[at : at + 128], 0.0), 0, keepdims=True)
            for at in range(0, column.shape[0], 128)
        ],
        1,
    )


def upright(line):
    eye = lax.broadcasted_iota(jnp.int32, (128, 128), 0) == lax.broadcasted_iota(
        jnp.int32, (128, 128), 1
    )
    return jnp.concatenate(
        [
            jnp.sum(jnp.where(eye, line[:, at : at + 128], 0.0), 1, keepdims=True)
            for at in range(0, line.shape[1], 128)
        ],
        0,
    )


def of_own_task(rows, task, weights):
    out = dot(rows, weights[0], ((1,), (0,)))
    for k in range(1, weights.shape[0]):
        out = jnp.where(task == k, dot(rows, weights[k], ((1,), (0,))), out)
    return out.astype(BF16)


def copies_kernel(x, out):
    rows = jnp.concatenate([x[k].astype(F32) for k in range(x.shape[0])]).astype(BF16)
    for k in range(out.shape[0]):
        out[k] = rows


def early_kernel(place, feats, mine, weights, rows, every_out, keys_out):
    depth, own = weights.shape[1], feats.shape[0] // 2
    for at, start in enumerate((place[1], 1 - place[1])):
        rows[at * own : (at + 1) * own] = feats[pl.ds(pl.multiple_of(start * own, own), own), :]
    keys_out[...] = of_own_task(mine[:, :depth], mine[:, depth : depth + 1].astype(F32), weights)
    for k in range(weights.shape[0]):
        every_out[k] = dot(rows[...], weights[k], ((1,), (0,))).astype(BF16)


def equal(a, b):
    return jnp.where(a == b, 1.0, 0.0)


def split(x):
    high = x.astype(BF16)
    rest = x - high.astype(F32)
    middle = rest.astype(BF16)
    return high, middle, (rest - middle.astype(F32)).astype(BF16)


def slots_of(slot, first, count):
    at = lax.broadcasted_iota(jnp.int32, (count, slot.shape[1]), 0) + first
    return equal(at.astype(F32), slot).astype(BF16)


def packed(dots, task, key_task, slot, first, count):
    pick = slots_of(slot, first, count)
    parts = split(jnp.where(task == key_task, dots, 0.0))
    out = dot(jnp.concatenate([pick] * 3, 1), jnp.concatenate(parts, 1), ((1,), (1,)))
    half = out.shape[1] // 2
    return jnp.concatenate([out[:, half:], out[:, :half]], 1)


def unpacked(slots, slot, first):
    pick = slots_of(slot, first, slots.shape[0])
    lanes = pl.cdiv(slots.shape[0], 128) * 128 - slots.shape[0]
    if lanes:
        slots = jnp.concatenate([slots, jnp.zeros((lanes, slots.shape[1]), F32)])
        pick = jnp.concatenate([pick, jnp.zeros((lanes, pick.shape[1]), BF16)])
    parts = jnp.concatenate(split(slots.T), 1)
    return dot(parts, jnp.concatenate([pick] * 3), ((1,), (0,)))


def index_of_keys(place, per, n_keys):
    half = n_keys // 2
    at = lax.broadcasted_iota(jnp.int32, (1, n_keys), 1)
    inside = lax.rem(at, half)
    key_core = jnp.where(at < half, place[0], 1 - place[0])
    return ((2 * lax.div(inside, per) + key_core) * per + lax.rem(inside, per)).astype(F32)


def late_kernel(
    per, place, positive, mine, theirs, mine_proj, every, weights,
    dots_out, message, query_out, keys_out, columns, lines, count_out,
):
    depth, n_query = weights.shape[1], dots_out.shape[0]
    half, own = mine.shape[0], n_query // 2
    keys_out[:half] = mine_proj[...]
    keys_out[half:] = of_own_task(
        theirs[:, :depth], theirs[:, depth : depth + 1].astype(F32), weights
    )
    upright_task = jnp.concatenate(
        [mine[:, depth : depth + 1].astype(F32), theirs[:, depth : depth + 1].astype(F32)]
    )
    key_task = jnp.concatenate(
        [lane_dense(mine[:, depth:].astype(F32)), lane_dense(theirs[:, depth:].astype(F32))], 1
    )
    before = lax.broadcasted_iota(jnp.int32, (2 * half, 2 * half), 0) < lax.broadcasted_iota(
        jnp.int32, (2 * half, 2 * half), 1
    )
    slot = jnp.sum(
        jnp.where(before, equal(upright_task, key_task), 0.0), 0, keepdims=True
    )
    count_out[0] = (jnp.max(slot) + 1.0).astype(jnp.int32)
    line = positive[...].astype(F32)
    pos = upright(
        jnp.where(place[1] == 0, line, jnp.concatenate([line[:, own:], line[:, :own]], 1))
    )
    chosen = pos == index_of_keys(place, per, 2 * half)
    task = jnp.sum(jnp.where(chosen, key_task, 0.0), 1, keepdims=True)
    first = lax.broadcasted_iota(jnp.int32, columns.shape, 1) == 0
    columns[...] = jnp.where(first, task, pos)
    query = every[0].astype(F32)
    for k in range(1, weights.shape[0]):
        query = jnp.where(task == k, every[k].astype(F32), query)
    query_out[...] = query.astype(BF16)
    keys = keys_out[...]
    wide = keys.astype(F32)
    query_sq = lane_dense(jnp.sum(query * query, 1, keepdims=True))
    key_sq = lane_dense(jnp.sum(wide * wide, 1, keepdims=True))
    dots = dot(query_out[...], keys, ((1,), (1,)))
    dots_out[...] = dots
    at = lax.broadcasted_iota(jnp.int32, lines.shape, 0)
    lines[...] = jnp.where(
        at == 0,
        jnp.concatenate([lane_dense(task), key_task], 1),
        jnp.where(
            at == 1,
            jnp.concatenate([query_sq, slot], 1),
            jnp.concatenate([query_sq, key_sq], 1),
        ),
    )
    n_slots = message.shape[0] - 8
    message[:n_slots] = packed(dots, task, key_task, slot, 0, n_slots)
    at = lax.broadcasted_iota(jnp.int32, (8, n_query), 0)
    swapped_sq = jnp.concatenate([query_sq[:, own:], query_sq[:, :own]], 1)
    message[n_slots:] = jnp.where(
        at == 0, swapped_sq, jnp.where(at == 1, key_sq[:, :half], key_sq[:, half:])
    )


def overflow_kernel(n_slots, dots, columns, lines, out):
    n_query = dots.shape[0]
    out[...] = packed(
        dots[...],
        columns[:, :1],
        lines[0:1, n_query:],
        lines[1:2, n_query:],
        n_slots,
        out.shape[0],
    )


def contrast_kernel(
    per, place, count, task_scale, dots, got, over, columns, lines, query_proj, key_proj,
    loss_out, back, full,
):
    n_query, n_keys = dots.shape
    own, n_slots = n_query // 2, got.shape[0] - 8
    task, pos = columns[:, :1], columns[:, 1:2]
    key_task, slot = lines[0:1, n_query:], lines[1:2, n_query:]
    full[...] = dots[...] + unpacked(got[:n_slots], slot, 0)

    @pl.when(count[0] > n_slots)
    def _():
        full[...] += unpacked(over[...], slot, n_slots)

    query_sq = lines[1:2, :n_query] + got[n_slots : n_slots + 1]
    key_sq = lines[2:3, n_query:] + jnp.concatenate(
        [got[n_slots + 1 : n_slots + 2], got[n_slots + 2 : n_slots + 3]], 1
    )
    key_line = 1.0 / jnp.sqrt(key_sq + EPS)
    query_inv, key_inv = upright(1.0 / jnp.sqrt(query_sq + EPS)), upright(key_line)
    scale = jnp.full(task.shape, task_scale[0], F32)
    for k in range(1, task_scale.shape[0]):
        scale = jnp.where(task == k, task_scale[k], scale)
    whole = full[...]
    half_cos = whole * key_line
    scores = half_cos * (scale * query_inv)
    expo = jnp.where(task == key_task, jnp.exp(scores), 0.0)
    chosen = pos == index_of_keys(place, per, n_keys)
    total = jnp.sum(expo, 1, keepdims=True)
    picked = jnp.sum(jnp.where(chosen, scores, 0.0), 1, keepdims=True)
    loss_out[...] = lane_dense((jnp.log(total) - picked)[:own])
    grads = scale * (expo * (1.0 / total) - jnp.where(chosen, 1.0, 0.0))
    grads = grads.astype(BF16)
    wide = grads.astype(F32)
    query_inner = jnp.sum(wide * half_cos, 1, keepdims=True)
    key_inner = upright(jnp.sum(wide * whole * query_inv, 0, keepdims=True))
    query_values, key_values = query_proj[...].astype(F32), key_proj[...].astype(F32)
    query_back = dot(grads, (key_values * key_inv).astype(BF16), ((1,), (0,)))
    key_back = dot(grads, (query_values * query_inv).astype(BF16), ((0,), (0,)))

    def through(values, inverse, grad, inner):
        return (inverse * grad - (inverse * inverse * inverse * inner) * values).astype(BF16)

    back[:n_query] = through(query_values, query_inv, query_back, query_inner)
    back[n_query:] = through(key_values, key_inv, key_back, key_inner)


def spread_kernel(width, n_tasks, place, rows, mine, theirs, task, away, here):
    depth = rows.shape[1]
    half, lines = depth // 2, away.shape[0] // 2
    line = lax.broadcasted_iota(jnp.int32, (lines, 1), 0)
    block = lax.div(line, n_tasks * width)
    r = lax.div(lax.rem(line, n_tasks * width), n_tasks)
    line_task = lax.rem(line, n_tasks).astype(F32)
    same = line_task == task[:1, :]
    for out, core in ((away, 1 - place[0]), (here, place[0])):
        column = (2 * block + core) * width + r
        pick = (column == lax.broadcasted_iota(jnp.int32, (lines, half), 1)).astype(F32).astype(BF16)
        for h in range(2):
            at = 0
            for part in (rows, mine, theirs):
                n = part.shape[0]
                got = dot(pick, part[:, h * half : (h + 1) * half], ((1,), (1,)))
                got = jnp.where(same[:, at : at + n], got, 0.0)
                out[h * lines : (h + 1) * lines, at : at + n] = got.astype(BF16)
                at += n


def in_vmem(n):
    return [pl.BlockSpec(memory_space=pltpu.SMEM)] + [pl.BlockSpec(memory_space=pltpu.VMEM)] * n


SLOTS = 176
ROOM = pltpu.CompilerParams(vmem_limit_bytes=16 << 20)


def cost(flops, moved):
    return pl.CostEstimate(flops=flops, bytes_accessed=moved, transcendentals=0)


def per_device(query_feats, key_feats, key_task, positive, head_weights, task_scale):
    core, member = lax.axis_index(CORE), lax.axis_index("tensor")
    n_tasks, depth, width = head_weights.shape
    n_query = query_feats.shape[0]
    own = n_query // 2
    n_far = lax.axis_size(FAR)
    per = key_feats.shape[0]
    out_rows = depth // (2 * n_far)

    tasks_in = jnp.broadcast_to(key_task.astype(BF16)[:, None], (per, 128))
    sent = jnp.concatenate([key_feats, tasks_in], 1)
    sent = jnp.broadcast_to(sent[None], (lax.axis_size(LINE), *sent.shape))
    place = jnp.stack([core, member])
    sent, place, positive = lax.optimization_barrier((sent, place, positive[None]))
    sent = lax.all_to_all(sent, LINE, 0, 0, tiled=True)
    sent = pl.pallas_call(
        copies_kernel,
        out_shape=jax.ShapeDtypeStruct(
            (lax.axis_size(PLANE), sent.shape[0] * per, depth + 128), BF16
        ),
        in_specs=in_vmem(1)[1:],
        out_specs=in_vmem(1)[1],
        compiler_params=ROOM,
        cost_estimate=cost(1 << 33, 1 << 20),
    )(sent)
    sent = lax.all_to_all(sent, PLANE, 0, 0, tiled=True).reshape(-1, depth + 128)
    arrived = sent
    arrived, place, positive = lax.optimization_barrier((arrived, place, positive))
    theirs = swapped(arrived, CORE)
    n_half = n_far * per
    n_keys = 2 * n_half

    feats, every, mine_proj = pl.pallas_call(
        early_kernel,
        out_shape=(
            jax.ShapeDtypeStruct((n_query, depth), BF16),
            jax.ShapeDtypeStruct((n_tasks, n_query, width), BF16),
            jax.ShapeDtypeStruct((n_half, width), BF16),
        ),
        in_specs=in_vmem(3),
        compiler_params=ROOM,
        out_specs=tuple(in_vmem(3)[1:]),
        cost_estimate=cost(2 * n_tasks * (n_query + n_half) * depth * width, 6 << 20),
    )(place, query_feats, arrived, head_weights)
    dots, message, query_proj, key_proj, columns, lines, count = pl.pallas_call(
        functools.partial(late_kernel, per),
        out_shape=(
            jax.ShapeDtypeStruct((n_query, n_keys), F32),
            jax.ShapeDtypeStruct((SLOTS + 8, n_query), F32),
            jax.ShapeDtypeStruct((n_query, width), BF16),
            jax.ShapeDtypeStruct((n_keys, width), BF16),
            jax.ShapeDtypeStruct((n_query, 128), F32),
            jax.ShapeDtypeStruct((8, n_query + n_keys), F32),
            jax.ShapeDtypeStruct((1,), jnp.int32),
        ),
        in_specs=in_vmem(6),
        out_specs=tuple(in_vmem(6)[1:] + in_vmem(0)),
        compiler_params=ROOM,
        cost_estimate=cost(2 * n_tasks * n_half * depth * width, 6 << 20),
    )(place, positive, arrived, theirs, mine_proj, every, head_weights)
    got = swapped(message, "tensor")

    def follow(operands):
        rest = pl.pallas_call(
            functools.partial(overflow_kernel, SLOTS),
            out_shape=jax.ShapeDtypeStruct((n_keys - SLOTS, n_query), F32),
            in_specs=in_vmem(3)[1:],
            out_specs=in_vmem(1)[1],
            compiler_params=ROOM,
        )(*operands)
        return swapped(rest, "tensor")

    def nothing(operands):
        return jnp.zeros((n_keys - SLOTS, n_query), F32)

    over = lax.cond(count[0] > SLOTS, follow, nothing, (dots, columns, lines))

    n_lines = n_far * n_tasks * out_rows
    away_feats, my_feats = pl.pallas_call(
        functools.partial(spread_kernel, out_rows, n_tasks),
        out_shape=(jax.ShapeDtypeStruct((n_lines, n_query + n_keys), BF16),) * 2,
        in_specs=in_vmem(4),
        out_specs=tuple(in_vmem(2)[1:]),
        compiler_params=ROOM,
        cost_estimate=cost(2 * n_lines * (n_query + n_keys) * depth, 6 << 20),
    )(place, feats, arrived, theirs, lines)
    query_loss, back = pl.pallas_call(
        functools.partial(contrast_kernel, per),
        out_shape=(
            jax.ShapeDtypeStruct((1, own), F32),
            jax.ShapeDtypeStruct((n_query + n_keys, width), BF16),
        ),
        in_specs=in_vmem(0) * 3 + in_vmem(7)[1:],
        out_specs=tuple(in_vmem(2)[1:]),
        scratch_shapes=[pltpu.VMEM((n_query, n_keys), F32)],
        compiler_params=ROOM,
        cost_estimate=cost(20 * n_query * n_keys * width, 6 << 20),
    )(place, count, task_scale, dots, got, over, columns, lines, query_proj, key_proj)
    query_loss = query_loss.reshape(own)

    away = dot(away_feats, back, ((1,), (0,))).astype(BF16)
    mine = lax.optimization_barrier(dot(my_feats, back, ((1,), (0,))))
    mine = mine + swapped(away, CORE).astype(F32)
    n_plane, n_line = lax.axis_size(PLANE), lax.axis_size(LINE)
    blocks = mine.astype(BF16).reshape(n_plane, -1, width)
    blocks, query_loss = lax.optimization_barrier((blocks, query_loss))
    arrived = lax.all_to_all(blocks, PLANE, 0, 0, tiled=True)
    blocks = sum(arrived[k].astype(F32) for k in range(n_plane))
    blocks = blocks.astype(BF16).reshape(n_line, -1, width)
    arrived = lax.all_to_all(blocks, LINE, 0, 0, tiled=True)
    weight_grad = jnp.sum(arrived.astype(F32), 0).reshape(out_rows, n_tasks, width)
    weight_grad = weight_grad.transpose(1, 0, 2)
    return (query_loss, weight_grad)


def solution(mesh):
    split = Mesh(
        mesh.devices.reshape(4, 2, 8, 2, mesh.shape["tensor"]),
        DP_TENSOR,
    )
    return jax.shard_map(
        per_device,
        mesh=split,
        in_specs=(P(DP, None), P(DP, None), P(DP), P(DP), P(None, None, "tensor"), P()),
        out_specs=(P(DP_TENSOR), P(None, DP, "tensor")),
        check_vma=False,
    )
```
